64 devices in a mesh: rep: 4 (over x, y), data: 16 (over z, core).
Axes of the slice: x: 2, y: 2, z: 8, core: 2. Of those that a mesh axis runs over, the one named last changes fastest.
The devices are a block of a 4x4x8 slice.
Arguments:
- x: bfloat16 [4096, 4096], P(('rep', 'data')), parts along dimension 0
- adapter_id: int32 [4096], P(('rep', 'data')), parts along dimension 0
- w_gate: bfloat16 [4096, 14336], replicated
- w_up: bfloat16 [4096, 14336], replicated
- w_down: bfloat16 [14336, 4096], replicated
- a_gate: bfloat16 [256, 8, 4096], P('data')
- b_gate: bfloat16 [256, 8, 14336], P('data')
- a_up: bfloat16 [256, 8, 4096], P('data')
- b_up: bfloat16 [256, 8, 14336], P('data')
- a_down: bfloat16 [256, 8, 14336], P('data')
- b_down: bfloat16 [256, 8, 4096], P('data')
Outputs:
- output: bfloat16 [4096, 4096], P(('rep', 'data')), parts along dimension 0
There are 4 independent parts. The reference program is written for one: setup_inputs(seed, part) draws one part's arguments, and reference() takes and returns one part's arrays. A program takes and returns all parts, laid end to end along the dimension named above; an argument that names none is the same for every part.
All inputs are finite; a program needn't handle non-finite values.
Results may differ from the reference program's by a relative error of at most 0.00571077.
Values are sent between devices in bfloat16 or wider.
A program may use at most 768 MiB of HBM per device.

```python
import jax
import jax.numpy as jnp
from jax import lax

D = 4096
FF = 14336
RANK = 8
ADAPTERS = 256
TOK = 64
GROUP = 16
CAP = 12
LORA_ALPHA = 32

SCALE = LORA_ALPHA / RANK
TOKENS = TOK * GROUP
PER_OWNER = ADAPTERS // GROUP


def shuffle_row(row_key, row_owner):
    return row_owner[jax.random.permutation(row_key, TOK)]


def draw_ids(id_key):
    id_keys = jax.random.split(id_key, 5)
    hot_owner = jax.random.randint(id_keys[0], (), 0, GROUP)
    offset = jax.random.randint(id_keys[1], (), 0, GROUP - 1)
    source = jnp.arange(GROUP)[:, None]
    position = jnp.arange(TOK)[None, :]
    spread = (offset + source * (TOK - CAP) + position - CAP) % (GROUP - 1)
    owner_idx = jnp.where(position < CAP, hot_owner, (hot_owner + 1 + spread) % GROUP)
    owner_idx = jax.vmap(shuffle_row)(jax.random.split(id_keys[2], GROUP), owner_idx)
    flat_owner = owner_idx.reshape(TOKENS)
    owner_hot = (flat_owner[:, None] == jnp.arange(GROUP)[None, :]).astype(jnp.int32)
    arrival = jnp.sum(jnp.cumsum(owner_hot, axis=0) * owner_hot, axis=1) - 1
    popular = jnp.minimum(jax.random.randint(id_keys[3], (TOKENS,), 0, PER_OWNER), jax.random.randint(id_keys[4], (TOKENS,), 0, PER_OWNER))
    local_idx = jnp.where(arrival == 0, 0, jnp.where(arrival == 1, PER_OWNER - 1, popular))
    return (flat_owner * PER_OWNER + local_idx).astype(jnp.int32)


def setup_inputs(seed: int = 0, part: int = 0) -> dict:
    key = jax.random.key(seed)
    weight_keys = jax.random.split(key, 9)
    part_keys = jax.random.split(jax.random.fold_in(key, part), 2)
    b_scale = 0.3 / (SCALE * RANK ** 0.5)

    def draw_normal(index, shape, std):
        return (jax.random.normal(weight_keys[index], shape, jnp.float32) * std).astype(jnp.bfloat16)

    return {
        "x": jax.random.normal(part_keys[0], (TOKENS, D), jnp.float32).astype(jnp.bfloat16),
        "adapter_id": draw_ids(part_keys[1]),
        "w_gate": draw_normal(0, (D, FF), D ** -0.5),
        "w_up": draw_normal(1, (D, FF), D ** -0.5),
        "w_down": draw_normal(2, (FF, D), FF ** -0.5),
        "a_gate": draw_normal(3, (ADAPTERS, RANK, D), D ** -0.5),
        "b_gate": draw_normal(4, (ADAPTERS, RANK, FF), b_scale),
        "a_up": draw_normal(5, (ADAPTERS, RANK, D), D ** -0.5),
        "b_up": draw_normal(6, (ADAPTERS, RANK, FF), b_scale),
        "a_down": draw_normal(7, (ADAPTERS, RANK, FF), FF ** -0.5),
        "b_down": draw_normal(8, (ADAPTERS, RANK, D), b_scale),
    }


def lora_delta(tok_rows, tok_ids, a_mat, b_mat):
    a_rows = a_mat[tok_ids].astype(jnp.float32)
    b_rows = b_mat[tok_ids].astype(jnp.float32)
    low_rank = jnp.einsum("td,trd->tr", tok_rows.astype(jnp.float32), a_rows).astype(jnp.bfloat16)
    full_rows = jnp.einsum("tr,trf->tf", low_rank.astype(jnp.float32), b_rows)
    return (SCALE * full_rows).astype(jnp.bfloat16)


def reference(x, adapter_id, w_gate, w_up, w_down, a_gate, b_gate, a_up, b_up, a_down, b_down):
    def one_block(block_in):
        tok_rows, tok_ids = block_in
        gate_pre = jnp.dot(tok_rows, w_gate, preferred_element_type=jnp.float32) + lora_delta(tok_rows, tok_ids, a_gate, b_gate).astype(jnp.float32)
        up_pre = jnp.dot(tok_rows, w_up, preferred_element_type=jnp.float32) + lora_delta(tok_rows, tok_ids, a_up, b_up).astype(jnp.float32)
        hidden = (jax.nn.silu(gate_pre) * up_pre).astype(jnp.bfloat16)
        down_out = jnp.dot(hidden, w_down, preferred_element_type=jnp.float32) + lora_delta(hidden, tok_ids, a_down, b_down).astype(jnp.float32)
        return (tok_rows.astype(jnp.float32) + down_out).astype(jnp.bfloat16)

    blocks = (x.reshape(GROUP, TOK, D), adapter_id.reshape(GROUP, TOK))
    return lax.map(one_block, blocks).reshape(TOKENS, D)
```

```python
import functools

import jax
import jax.numpy as jnp
from jax import lax
from jax.experimental import pallas as pl
from jax.experimental.pallas import tpu as pltpu
from jax.sharding import PartitionSpec as P

ALPHA = 32
MESH = pl.DeviceIdType.MESH
BF16, F32 = jnp.bfloat16, jnp.float32
SUB = 512
LANES = 128
PACK = 4
HELD = 9
SLOTS = 24
AHEAD = 3


def nt_dot(a, b):
    return lax.dot_general(a, b, (((1,), (1,)), ((), ())), preferred_element_type=F32)


def dot(a, b):
    return jnp.dot(a, b, preferred_element_type=F32)


def layer_kernel(
    groups, cap, scale, per_owner, rank,
    x_hbm, ids_ref, wg_hbm, wu_hbm, wd_hbm, ag_hbm, bg_hbm, au_hbm, bu_hbm, ad_hbm, bd_hbm,
    out_hbm,
    x_own, send, mask_send, recv, mask_recv, xs, acc, hid, wbuf, abuf, lbuf, bdbuf,
    low, lowm, lowd, oacc, back_send, back_recv, out_own, pick,
    w_sem, misc_sem, a_sem, l_sem, xs_send, xs_recv, m_send, m_recv, b_send, b_recv, o_sem,
):
    tok, width = x_own.shape
    rows = groups * cap
    wide = wg_hbm.shape[1]
    ranks = per_owner * rank
    tile = 2 * SUB
    n_chunk = width // SUB
    n_tile = wide // tile
    n_out = width // SUB
    per_msg = cap // PACK
    blocks = SUB // LANES
    n_step1 = n_chunk * n_tile
    n_step2 = n_out * n_tile
    n_block = 2 * n_step1 + n_step2

    me = lax.axis_index("data")
    peers = [2 * (groups // 4) + k for k in (0, 1)]
    order = []
    for d in range(groups // 4, 0, -1):
        order += [2 * d, 2 * d + 1, groups - 2 * d, groups - 2 * d + 1]
    seen = []
    for off in order + list(range(groups)):
        off = off % groups
        if off and off not in seen:
            seen.append(off)
    peers = [lax.rem(me + off, groups) for off in seen]

    def w_copies(b):
        slot = lax.rem(b, SLOTS)
        return slot

    def start_w1(step, b):
        early = step < HELD * n_chunk
        late = step - HELD * n_chunk
        c = jnp.where(early, step // HELD, lax.rem(late, n_chunk))
        n = jnp.where(early, lax.rem(step, HELD), HELD + late // n_chunk)
        k0 = pl.multiple_of(c * SUB, SUB)
        n0 = pl.multiple_of(n * tile, tile)
        for which, w in enumerate((wg_hbm, wu_hbm)):
            slot = lax.rem(b + which, SLOTS)
            for half in range(2):
                pltpu.make_async_copy(
                    w.at[pl.ds(k0, SUB), pl.ds(n0 + half * SUB, SUB)], wbuf.at[slot, half], w_sem.at[slot]
                ).start()

    def start_w2(step, b):
        j = step // n_tile
        k = lax.rem(step, n_tile)
        slot = lax.rem(b, SLOTS)
        n0 = pl.multiple_of(j * SUB, SUB)
        for half in range(2):
            k0 = pl.multiple_of(k * tile + half * SUB, SUB)
            pltpu.make_async_copy(
                wd_hbm.at[pl.ds(k0, SUB), pl.ds(n0, SUB)], wbuf.at[slot, half], w_sem.at[slot]
            ).start()

    def wait_w(slot):
        pltpu.make_async_copy(wbuf.at[slot], wbuf.at[slot], w_sem.at[slot]).wait()

    def l_copies(n):
        s = lax.rem(n, 2)
        n0 = pl.multiple_of(n * tile, tile)
        return [
            pltpu.make_async_copy(src.at[:, pl.ds(n0, tile)], lbuf.at[s, i], l_sem.at[s])
            for i, src in enumerate((bg_hbm, bu_hbm, ad_hbm))
        ]

    x_copy = pltpu.make_async_copy(x_hbm, x_own, misc_sem.at[0])
    bd_copy = pltpu.make_async_copy(bd_hbm, bdbuf, misc_sem.at[1])
    x_copy.start()
    for i in range(2):
        for c in range(n_chunk):
            src = (ag_hbm, au_hbm)[i]
            pltpu.make_async_copy(
                src.at[:, pl.ds(c * SUB, SUB)], abuf.at[c, pl.ds(i * ranks, ranks)], a_sem.at[c]
            ).start()

    @pl.loop(0, SLOTS // 2)
    def _(s):
        start_w1(s, 2 * s)

    bd_copy.start()
    for n in range(2):
        for cp in l_copies(n):
            cp.start()

    barrier = pltpu.get_barrier_semaphore()
    for peer in peers:
        pl.semaphore_signal(barrier, inc=1, device_id={"data": peer}, device_id_type=MESH)

    ids = ids_ref[...].astype(F32)
    r0 = lax.broadcasted_iota(jnp.int32, (tok, tok), 0).astype(F32)
    r1 = lax.broadcasted_iota(jnp.int32, (tok, tok), 1).astype(F32)
    ids_row = jnp.broadcast_to(ids, (tok, tok))
    ids_col = jnp.broadcast_to(jnp.sum(jnp.where(r0 == r1, ids_row, 0.0), axis=1, keepdims=True), (tok, tok))
    own_row = jnp.floor((ids_row + 0.5) * (1.0 / per_owner))
    own_col = jnp.floor((ids_col + 0.5) * (1.0 / per_owner))
    same = own_row == own_col
    arr_row = jnp.sum(jnp.where(same & (r0 < r1), 1.0, 0.0), axis=0, keepdims=True)
    arr_col = jnp.sum(jnp.where(same & (r1 < r0), 1.0, 0.0), axis=1, keepdims=True)
    slot_row = own_row[:1, :] * cap + arr_row
    slot_col = own_col[:, :1] * cap + arr_col
    loc_col = ids_col[:, :1] - own_col[:, :1] * per_owner
    s_row = lax.broadcasted_iota(jnp.int32, (rows, tok), 0).astype(F32)
    spread = jnp.where(s_row == jnp.broadcast_to(slot_row, (rows, tok)), 1.0, 0.0).astype(BF16)
    s_col = lax.broadcasted_iota(jnp.int32, (tok, rows), 1).astype(F32)
    pick[...] = jnp.where(s_col == jnp.broadcast_to(slot_col, (tok, rows)), 1.0, 0.0).astype(BF16)
    lane = lax.broadcasted_iota(jnp.int32, (tok, ranks), 1).astype(F32)
    lane_ad = jnp.floor((lane + 0.5) * (1.0 / rank))
    mine = jnp.where(lane_ad == jnp.broadcast_to(loc_col, (tok, ranks)), 1.0, 0.0).astype(BF16)

    low[...] = jnp.zeros_like(low)
    lowd[...] = jnp.zeros_like(lowd)
    oacc[...] = jnp.zeros_like(oacc)

    mask_send[...] = dot(spread, mine).astype(BF16).reshape(mask_send.shape)
    x_copy.wait()
    for c in range(n_chunk):
        part = dot(spread, x_own[:, c * SUB:(c + 1) * SUB]).astype(BF16)
        for q in range(blocks):
            send[:, c * blocks + q] = part[:, q * LANES:(q + 1) * LANES].reshape(groups, per_msg, PACK, LANES)

    mine_at = pl.ds(per_msg * me, per_msg)

    def send_x(c):
        for peer in peers:
            pltpu.make_async_remote_copy(
                src_ref=send.at[peer, pl.ds(c * blocks, blocks)],
                dst_ref=recv.at[pl.ds(c * blocks, blocks), mine_at],
                send_sem=xs_send.at[c], recv_sem=xs_recv.at[c],
                device_id={"data": peer}, device_id_type=MESH,
            ).start()

    def send_out(j):
        for peer in peers:
            pltpu.make_async_remote_copy(
                src_ref=back_send.at[peer, pl.ds(j * blocks, blocks)],
                dst_ref=back_recv.at[pl.ds(j * blocks, blocks), mine_at],
                send_sem=b_send.at[j], recv_sem=b_recv.at[j],
                device_id={"data": peer}, device_id_type=MESH,
            ).start()

    def await_peers(buf, c, sem):
        view = buf.at[pl.ds(c * blocks, blocks), pl.ds(0, per_msg * (groups - 1))]
        pltpu.make_async_copy(view, view, sem).wait()

    def await_sent(buf, c, sem):
        view = buf.at[pl.ds(0, groups - 1), pl.ds(c * blocks, blocks)]
        pltpu.make_async_copy(view, view, sem).wait()

    @pl.loop(0, n_chunk * blocks)
    def _(q):
        recv[q, mine_at] = send[me, q]

    mask_recv[mine_at] = mask_send[mine_at]

    pl.semaphore_wait(barrier, groups - 1)

    @pl.loop(0, AHEAD)
    def _(c):
        send_x(c)

    @pl.loop(0, HELD)
    def _(n):
        acc[0, n] = jnp.zeros(acc.shape[2:], F32)
        acc[1, n] = jnp.zeros(acc.shape[2:], F32)

    def arrive(c):
        @pl.when(c + AHEAD < n_chunk)
        def _():
            send_x(c + AHEAD)

        @pl.when(c == n_chunk - AHEAD)
        def _():
            for peer in peers:
                pltpu.make_async_remote_copy(
                    src_ref=mask_send.at[pl.ds(per_msg * peer, per_msg)],
                    dst_ref=mask_recv.at[mine_at],
                    send_sem=m_send, recv_sem=m_recv,
                    device_id={"data": peer}, device_id_type=MESH,
                ).start()

        await_peers(recv, c, xs_recv.at[c])
        for q in range(blocks):
            xs[c, :, q * LANES:(q + 1) * LANES] = recv[c * blocks + q].reshape(rows, LANES)
        pltpu.make_async_copy(abuf.at[c], abuf.at[c], a_sem.at[c]).wait()
        low[...] += nt_dot(xs[c], abuf[c])

        @pl.when(c == n_chunk - 1)
        def _():
            view = mask_recv.at[pl.ds(0, per_msg * (groups - 1))]
            pltpu.make_async_copy(view, view, m_recv).wait()
            mask = mask_recv[...].reshape(rows, ranks).astype(F32) > 0.0
            for i in range(2):
                kept = low[:, i * ranks:(i + 1) * ranks].astype(BF16).astype(F32)
                lowm[i] = jnp.where(mask, kept, 0.0).astype(BF16)

    def delta(a, b):
        return (scale * dot(a, b)).astype(BF16).astype(F32)

    @pl.loop(0, n_step1)
    def _(step):
        early = step < HELD * n_chunk
        late = step - HELD * n_chunk
        c = jnp.where(early, step // HELD, lax.rem(late, n_chunk))
        n = jnp.where(early, lax.rem(step, HELD), HELD + late // n_chunk)
        a = lax.rem(n, HELD)

        @pl.when(early & (n == 0))
        def _():
            arrive(c)

        for which in range(2):
            slot = lax.rem(2 * step + which, SLOTS)
            wait_w(slot)
            for half in range(2):
                cols = slice(half * SUB, (half + 1) * SUB)
                acc[which, a, :, cols] += dot(xs[c], wbuf[slot, half])

        nxt = 2 * step + SLOTS

        @pl.when(nxt < 2 * n_step1)
        def _():
            start_w1(step + SLOTS // 2, nxt)

        @pl.when(nxt >= 2 * n_step1)
        def _():
            start_w2(nxt - 2 * n_step1, nxt)
            start_w2(nxt + 1 - 2 * n_step1, nxt + 1)

        @pl.when(c == n_chunk - 1)
        def _():
            s = lax.rem(n, 2)
            pltpu.make_async_copy(lbuf.at[s], lbuf.at[s], l_sem.at[s]).wait()
            piece = tile // 4
            for p in range(4):
                cols = slice(p * piece, (p + 1) * piece)
                g = acc[0, a, :, cols] + delta(lowm[0], lbuf[s, 0, :, cols])
                u = acc[1, a, :, cols] + delta(lowm[1], lbuf[s, 1, :, cols])
                hid[n, :, cols] = (jax.nn.silu(g) * u).astype(BF16)
            acc[0, a] = jnp.zeros(acc.shape[2:], F32)
            acc[1, a] = jnp.zeros(acc.shape[2:], F32)
            lowd[...] += nt_dot(hid[n], lbuf[s, 2])

            @pl.when(n + 2 < n_tile)
            def _():
                for cp in l_copies(n + 2):
                    cp.start()

    mask = mask_recv[...].reshape(rows, ranks).astype(F32) > 0.0
    lowm[0] = jnp.where(mask, lowd[...].astype(BF16).astype(F32), 0.0).astype(BF16)
    bd_copy.wait()

    def combine(j):
        await_peers(back_recv, j, b_recv.at[j])
        part = jnp.concatenate([back_recv[j * blocks + q].reshape(rows, LANES) for q in range(blocks)], axis=1)
        o0 = pl.multiple_of(j * SUB, SUB)
        out_own[j] = dot(pick[...], part).astype(BF16)
        pltpu.make_async_copy(out_own.at[j], out_hbm.at[:, pl.ds(o0, SUB)], o_sem).start()

    @pl.loop(0, n_step2)
    def _(step):
        j = step // n_tile
        k = lax.rem(step, n_tile)
        b = 2 * n_step1 + step
        slot = lax.rem(b, SLOTS)
        wait_w(slot)
        for half in range(2):
            oacc[...] += dot(hid[k, :, half * SUB:(half + 1) * SUB], wbuf[slot, half])

        @pl.when(b + SLOTS < n_block)
        def _():
            start_w2(step + SLOTS, b + SLOTS)

        @pl.when((k == 1) & (j > 0))
        def _():
            send_out(j - 1)

        @pl.when((k == n_tile - 2) & (j > 1))
        def _():
            combine(j - 2)

        @pl.when(k == n_tile - 1)
        def _():
            o0 = pl.multiple_of(j * SUB, SUB)
            total = xs[j].astype(F32) + (oacc[...] + delta(lowm[0], bdbuf[:, pl.ds(o0, SUB)]))
            oacc[...] = jnp.zeros_like(oacc)
            row = total.astype(BF16)
            for q in range(blocks):
                back_send[:, j * blocks + q] = row[:, q * LANES:(q + 1) * LANES].reshape(
                    groups, per_msg, PACK, LANES)
            for q in range(blocks):
                back_recv[j * blocks + q, mine_at] = back_send[me, j * blocks + q]

    send_out(n_out - 1)
    combine(n_out - 2)
    combine(n_out - 1)

    for c in range(n_chunk):
        await_sent(send, c, xs_send.at[c])
    view = mask_send.at[pl.ds(0, per_msg * (groups - 1))]
    pltpu.make_async_copy(view, view, m_send).wait()
    for j in range(n_out):
        await_sent(back_send, j, b_send.at[j])
    pltpu.make_async_copy(out_own, out_own, o_sem).wait()


def solution(mesh):
    groups = mesh.shape["data"]
    row_spec = P(("rep", "data"), None)
    id_spec = P(("rep", "data"))
    owned_spec = P("data", None, None)

    def device_step(x, adapter_id, w_gate, w_up, w_down, a_gate, b_gate, a_up, b_up, a_down, b_down):
        tok, width = x.shape
        wide = w_gate.shape[1]
        per_owner, rank = a_gate.shape[:2]
        cap = (3 * tok + groups - 1) // groups
        rows, ranks, tile = groups * cap, per_owner * rank, 2 * SUB
        per_msg, n_chunk, n_tile = cap // PACK, width // SUB, wide // tile
        assert cap % PACK == 0 and width % SUB == 0 and wide % tile == 0 and ranks == LANES

        def flat(m):
            return m.reshape(ranks, m.shape[2])

        vm = pltpu.VMEM
        any_spec = pl.BlockSpec(memory_space=pl.ANY)
        msg = (groups, width // LANES, per_msg, PACK, LANES)
        got = (width // LANES, groups * per_msg, PACK, LANES)
        small = (groups * per_msg, PACK, LANES)
        dma = pltpu.SemaphoreType.DMA
        return pl.pallas_call(
            functools.partial(layer_kernel, groups, cap, ALPHA / rank, per_owner, rank),
            out_shape=jax.ShapeDtypeStruct((tok, width), BF16),
            in_specs=[any_spec, pl.BlockSpec(memory_space=pltpu.VMEM)] + [any_spec] * 9,
            out_specs=any_spec,
            scratch_shapes=[
                vm((tok, width), BF16), vm(msg, BF16), vm(small, BF16), vm(got, BF16), vm(small, BF16),
                vm((n_chunk, rows, SUB), BF16), vm((2, HELD, rows, tile), F32), vm((n_tile, rows, tile), BF16),
                vm((SLOTS, 2, SUB, SUB), BF16), vm((n_chunk, 2 * ranks, SUB), BF16), vm((2, 3, ranks, tile), BF16),
                vm((ranks, width), BF16), vm((rows, 2 * ranks), F32), vm((2, rows, ranks), BF16),
                vm((rows, ranks), F32), vm((rows, SUB), F32), vm(msg, BF16), vm(got, BF16),
                vm((width // SUB, tok, SUB), BF16), vm((tok, rows), BF16),
                dma((SLOTS,)), dma((2,)), dma((n_chunk,)), dma((2,)), dma((n_chunk,)), dma((n_chunk,)), dma, dma,
                dma((width // SUB,)), dma((width // SUB,)), dma,
            ],
            compiler_params=pltpu.CompilerParams(
                collective_id=0, has_side_effects=True, vmem_limit_bytes=67043328),
            name="owner_layer",
        )(x, adapter_id.reshape(1, tok), w_gate, w_up, w_down, flat(a_gate), flat(b_gate), flat(a_up), flat(b_up),
          flat(a_down), flat(b_down))

    return jax.shard_map(
        device_step, mesh=mesh,
        in_specs=(row_spec, id_spec, P(), P(), P()) + (owned_spec,) * 6,
        out_specs=row_spec, check_vma=False)
```

```python
import functools

import jax
import jax.numpy as jnp
from jax import lax
from jax.experimental import pallas as pl
from jax.experimental.pallas import tpu as pltpu
from jax.sharding import PartitionSpec as P

ALPHA = 32
MESH = pl.DeviceIdType.MESH
BF16, F32 = jnp.bfloat16, jnp.float32
SUB = 512
LANES = 128
PACK = 4
HELD = 9
PAIRS = 12
LBUFS = 4


def nt_dot(a, b):
    return lax.dot_general(a, b, (((1,), (1,)), ((), ())), preferred_element_type=F32)


def dot(a, b):
    return jnp.dot(a, b, preferred_element_type=F32)


def layer_kernel(
    groups, cap, scale, per_owner, rank,
    x_hbm, ids_ref, wg_hbm, wu_hbm, wd_hbm, ag_hbm, bg_hbm, au_hbm, bu_hbm, ad_hbm, bd_hbm,
    out_hbm,
    x_own, send, mask_send, recv, mask_recv, xs, acc, hid, wbuf, abuf, lbuf, bdbuf,
    low, lowm, lowd, oacc, back_send, back_recv, out_own, pick,
    w_sem, misc_sem, a_sem, l_sem, xs_send, xs_recv, m_send, m_recv, b_send, b_recv, o_sem,
):
    tok, width = x_own.shape
    rows = groups * cap
    wide = wg_hbm.shape[1]
    ranks = per_owner * rank
    n_chunk = width // SUB
    n_tile = wide // SUB
    n_out = width // SUB
    per_msg = cap // PACK
    blocks = SUB // LANES
    n_held = 2 * HELD
    k_pair = 4 * SUB
    n_kp = wide // k_pair
    n_deep = n_chunk // 2
    messages = [(0, 1), (1, 1)] + [(c, 2) for c in range(2, n_chunk, 2)]

    me = lax.axis_index("data")
    seen = []
    for d in range(groups // 4, 0, -1):
        for off in (2 * d, 2 * d + 1, groups - 2 * d, groups - 2 * d + 1):
            if off % groups and off % groups not in seen:
                seen.append(off % groups)
    seen += [off for off in range(1, groups) if off not in seen]
    peers = [lax.rem(me + off, groups) for off in seen]

    def nxt(slot):
        return jnp.where(slot == PAIRS - 1, 0, slot + 1)

    def start_a1(slot, c, n):
        for which, w in enumerate((wg_hbm, wu_hbm)):
            for half in range(2):
                n0 = pl.multiple_of(n * (2 * SUB) + half * SUB, SUB)
                pltpu.make_async_copy(
                    w.at[pl.ds(c * SUB, SUB), pl.ds(n0, SUB)],
                    wbuf.at[slot, which, pl.ds(half * SUB, SUB)], w_sem.at[slot],
                ).start()

    def start_gu(slot, p, n):
        k0 = pl.multiple_of(p * (2 * SUB), 2 * SUB)
        n0 = pl.multiple_of(n * SUB, SUB)
        for which, w in enumerate((wg_hbm, wu_hbm)):
            pltpu.make_async_copy(
                w.at[pl.ds(k0, 2 * SUB), pl.ds(n0, SUB)], wbuf.at[slot, which], w_sem.at[slot]).start()

    def start_d(slot, j, kp):
        n0 = pl.multiple_of(j * SUB, SUB)
        for half in range(2):
            k0 = pl.multiple_of(kp * k_pair + half * 2 * SUB, 2 * SUB)
            pltpu.make_async_copy(
                wd_hbm.at[pl.ds(k0, 2 * SUB), pl.ds(n0, SUB)], wbuf.at[slot, half], w_sem.at[slot]).start()

    def wait_w(slot):
        pltpu.make_async_copy(wbuf.at[slot], wbuf.at[slot], w_sem.at[slot]).wait()

    def issue(i, slot):
        for count, start in (
            (2 * HELD, lambda i: start_a1(slot, i // HELD, i % HELD)),
            ((n_deep - 1) * n_held, lambda i: start_gu(slot, 1 + i // n_held, i % n_held)),
            ((n_tile - n_held) * n_deep, lambda i: start_gu(slot, i % n_deep, n_held + i // n_deep)),
            (n_out * n_kp, lambda i: start_d(slot, i // n_kp, i % n_kp)),
        ):
            if i < count:
                start(i)
                return
            i -= count

    kinds = []
    for o in range(2):
        kinds += [("a1", o, n) for n in range(HELD)]
    for o in range(1, n_deep):
        kinds += [("gu", o, n) for n in range(n_held)]
    for n in range(n_held, n_tile):
        kinds += [("gu", o, n) for o in range(n_deep)]
    for o in range(n_out):
        kinds += [("d", o, n) for n in range(n_kp)]
    starts = {"a1": start_a1, "gu": start_gu, "d": start_d}
    n_pair = len(kinds)

    def run(first, count, size, body):
        step = 0
        while step < count:
            def refill(s):
                return [kinds[q] if q < n_pair else None for q in
                        range(first + s * size + PAIRS, first + (s + 1) * size + PAIRS)]

            def rule(a, b):
                if any((p is None) != (q is None) or (p and p[0] != q[0]) for p, q in zip(a, b)):
                    return None
                return [p and (q[1] - p[1], q[2] - p[2]) for p, q in zip(a, b)]

            end = step + 1
            delta = None
            while end < count:
                d = rule(refill(end - 1), refill(end))
                if d is None or (delta is not None and d != delta):
                    break
                delta = d
                end += 1
            base = refill(step)
            slot0 = (first + step * size) % PAIRS

            def one(s, slot, base=base, delta=delta, step=step):
                slots = [slot]
                for _ in range(size - 1):
                    slots.append(nxt(slots[-1]))
                body(s, slots)
                for i, item in enumerate(base):
                    if item is None:
                        continue
                    kind, o, n = item
                    if delta is not None:
                        o, n = o + (s - step) * delta[i][0], n + (s - step) * delta[i][1]
                    starts[kind](slots[i], o, n)
                return nxt(slots[-1])

            if end - step == 1:
                one(step, slot0)
            else:
                lax.fori_loop(step, end, one, jnp.int32(slot0))
            step = end

    def l_copies(n, s):
        n0 = pl.multiple_of(n * SUB, SUB)
        return [
            pltpu.make_async_copy(src.at[:, pl.ds(n0, SUB)], lbuf.at[s, i], l_sem.at[s])
            for i, src in enumerate((bg_hbm, bu_hbm, ad_hbm))
        ]

    x_copy = pltpu.make_async_copy(x_hbm, x_own, misc_sem.at[0])
    bd_copy = pltpu.make_async_copy(bd_hbm, bdbuf, misc_sem.at[1])
    x_copy.start()
    for i in range(2):
        for c in range(n_chunk):
            src = (ag_hbm, au_hbm)[i]
            pltpu.make_async_copy(
                src.at[:, pl.ds(c * SUB, SUB)], abuf.at[c, pl.ds(i * ranks, ranks)], a_sem.at[c]
            ).start()

    barrier = pltpu.get_barrier_semaphore()
    for peer in peers:
        pl.semaphore_signal(barrier, inc=1, device_id={"data": peer}, device_id_type=MESH)

    for i in range(PAIRS):
        issue(i, i)
    for n in range(LBUFS):
        for cp in l_copies(n, n):
            cp.start()
    bd_copy.start()

    ids = ids_ref[...].astype(F32)
    r0 = lax.broadcasted_iota(jnp.int32, (tok, tok), 0).astype(F32)
    r1 = lax.broadcasted_iota(jnp.int32, (tok, tok), 1).astype(F32)
    ids_row = jnp.broadcast_to(ids, (tok, tok))
    ids_col = jnp.broadcast_to(jnp.sum(jnp.where(r0 == r1, ids_row, 0.0), axis=1, keepdims=True), (tok, tok))
    own_row = jnp.floor((ids_row + 0.5) * (1.0 / per_owner))
    own_col = jnp.floor((ids_col + 0.5) * (1.0 / per_owner))
    same = own_row == own_col
    arr_row = jnp.sum(jnp.where(same & (r0 < r1), 1.0, 0.0), axis=0, keepdims=True)
    arr_col = jnp.sum(jnp.where(same & (r1 < r0), 1.0, 0.0), axis=1, keepdims=True)
    slot_row = own_row[:1, :] * cap + arr_row
    slot_col = own_col[:, :1] * cap + arr_col
    loc_col = ids_col[:, :1] - own_col[:, :1] * per_owner
    s_row = lax.broadcasted_iota(jnp.int32, (rows, tok), 0).astype(F32)
    spread = jnp.where(s_row == jnp.broadcast_to(slot_row, (rows, tok)), 1.0, 0.0).astype(BF16)
    s_col = lax.broadcasted_iota(jnp.int32, (tok, rows), 1).astype(F32)
    pick[...] = jnp.where(s_col == jnp.broadcast_to(slot_col, (tok, rows)), 1.0, 0.0).astype(BF16)
    lane = lax.broadcasted_iota(jnp.int32, (tok, ranks), 1).astype(F32)
    lane_ad = jnp.floor((lane + 0.5) * (1.0 / rank))
    mine = jnp.where(lane_ad == jnp.broadcast_to(loc_col, (tok, ranks)), 1.0, 0.0).astype(BF16)

    mask_send[...] = dot(spread, mine).astype(BF16).reshape(mask_send.shape)
    x_copy.wait()
    for c in range(n_chunk):
        part = dot(spread, x_own[:, c * SUB:(c + 1) * SUB]).astype(BF16)
        for q in range(blocks):
            send[:, c * blocks + q] = part[:, q * LANES:(q + 1) * LANES].reshape(groups, per_msg, PACK, LANES)

    mine_at = pl.ds(per_msg * me, per_msg)

    def exchange(src, dst, first, count, send_sem, recv_sem):
        for peer in peers:
            pltpu.make_async_remote_copy(
                src_ref=src.at[peer, pl.ds(first, count)], dst_ref=dst.at[pl.ds(first, count), mine_at],
                send_sem=send_sem, recv_sem=recv_sem, device_id={"data": peer}, device_id_type=MESH,
            ).start()

    def send_out(j):
        exchange(back_send, back_recv, j * blocks, blocks, b_send.at[j], b_recv.at[j])

    def await_peers(buf, first, count, sem):
        view = buf.at[pl.ds(first, count), pl.ds(0, per_msg * (groups - 1))]
        pltpu.make_async_copy(view, view, sem).wait()

    def await_sent(buf, first, count, sem):
        view = buf.at[pl.ds(0, groups - 1), pl.ds(first, count)]
        pltpu.make_async_copy(view, view, sem).wait()

    @pl.loop(0, n_chunk * blocks)
    def _(q):
        recv[q, mine_at] = send[me, q]

    mask_recv[mine_at] = mask_send[mine_at]

    pl.semaphore_wait(barrier, groups - 1)

    for m, (c, count) in enumerate(messages):
        exchange(send, recv, c * blocks, count * blocks, xs_send.at[m], xs_recv.at[m])
    for peer in peers:
        pltpu.make_async_remote_copy(
            src_ref=mask_send.at[pl.ds(per_msg * peer, per_msg)], dst_ref=mask_recv.at[mine_at],
            send_sem=m_send, recv_sem=m_recv, device_id={"data": peer}, device_id_type=MESH,
        ).start()

    def arrive(m):
        first, count = messages[m]
        await_peers(recv, first * blocks, count * blocks, xs_recv.at[m])
        for c in range(first, first + count):
            for q in range(blocks):
                xs[c, :, q * LANES:(q + 1) * LANES] = recv[c * blocks + q].reshape(rows, LANES)
            pltpu.make_async_copy(abuf.at[c], abuf.at[c], a_sem.at[c]).wait()
            part = nt_dot(xs[c], abuf[c])
            low[...] = part if c == 0 else low[...] + part

    def masked(value):
        mask = mask_recv[...].reshape(rows, ranks).astype(F32) > 0.0
        return jnp.where(mask, value.astype(BF16).astype(F32), 0.0).astype(BF16)

    def delta(a, b):
        return (scale * dot(a, b)).astype(BF16).astype(F32)

    def deep(p):
        return jnp.concatenate([xs[2 * p], xs[2 * p + 1]], axis=1)

    def finish(n, s, gate, up):
        pltpu.make_async_copy(lbuf.at[s], lbuf.at[s], l_sem.at[s]).wait()
        for p in range(2):
            cols = slice(p * SUB // 2, (p + 1) * SUB // 2)
            g = gate(cols) + delta(lowm[0], lbuf[s, 0, :, cols])
            u = up(cols) + delta(lowm[1], lbuf[s, 1, :, cols])
            hid[n, :, cols] = (jax.nn.silu(g) * u).astype(BF16)
        lowd[...] += nt_dot(hid[n], lbuf[s, 2])

    at = 0
    for c in range(2):
        arrive(c)

        def shallow(n, slots, c=c):
            wait_w(slots[0])
            for which in range(2):
                for half in range(2):
                    part = dot(xs[c], wbuf[slots[0], which, half * SUB:(half + 1) * SUB])
                    if c == 0:
                        acc[which, 2 * n + half] = part
                    else:
                        acc[which, 2 * n + half] += part

        run(at, HELD, 1, shallow)
        at += HELD

    for p in range(1, n_deep):
        arrive(p + 1)
        last = p == n_deep - 1
        if last:
            view = mask_recv.at[pl.ds(0, per_msg * (groups - 1))]
            pltpu.make_async_copy(view, view, m_recv).wait()
            for i in range(2):
                lowm[i] = masked(low[:, i * ranks:(i + 1) * ranks])
            lowd[...] = jnp.zeros_like(lowd)

        def pair(n2, slots, p=p, last=last):
            for i in range(2):
                n = 2 * n2 + i
                wait_w(slots[i])
                for which in range(2):
                    acc[which, n] += dot(deep(p), wbuf[slots[i], which])
                if last:
                    s = lax.rem(n, LBUFS)
                    finish(n, s, lambda cols: acc[0, n, :, cols], lambda cols: acc[1, n, :, cols])
                    for cp in l_copies(n + LBUFS, s):
                        cp.start()

        run(at, HELD, 2, pair)
        at += n_held

    for with_copies, lo, hi in ((True, n_held, n_tile - LBUFS), (False, n_tile - LBUFS, n_tile)):

        def whole(step, slots, with_copies=with_copies, lo=lo):
            n = lo + step
            for slot in slots:
                wait_w(slot)
            for which in range(2):
                total = dot(deep(0), wbuf[slots[0], which])
                for p in range(1, n_deep):
                    total = total + dot(deep(p), wbuf[slots[p], which])
                acc[which, 0] = total
            s = lax.rem(n, LBUFS)
            finish(n, s, lambda cols: acc[0, 0, :, cols], lambda cols: acc[1, 0, :, cols])
            if with_copies:
                for cp in l_copies(n + LBUFS, s):
                    cp.start()

        run(at, hi - lo, n_deep, whole)
        at += (hi - lo) * n_deep

    lowm[0] = masked(lowd[...])
    bd_copy.wait()

    def combine(j):
        await_peers(back_recv, j * blocks, blocks, b_recv.at[j])
        part = jnp.concatenate([back_recv[j * blocks + q].reshape(rows, LANES) for q in range(blocks)], axis=1)
        o0 = pl.multiple_of(j * SUB, SUB)
        out_own[j] = dot(pick[...], part).astype(BF16)
        pltpu.make_async_copy(out_own.at[j], out_hbm.at[:, pl.ds(o0, SUB)], o_sem).start()

    def column(j, slots):
        cut = (n_kp + 1) // 2
        o0 = pl.multiple_of(j * SUB, SUB)
        for part, (lo, hi) in enumerate(((0, cut), (cut, n_kp))):
            total = None
            for kp in range(lo, hi):
                wait_w(slots[kp])
            for kp in range(lo, hi):
                for half in range(2):
                    h = 4 * kp + 2 * half
                    term = dot(jnp.concatenate([hid[h], hid[h + 1]], axis=1), wbuf[slots[kp], half])
                    total = term if total is None else total + term
            if part == 0:
                oacc[...] = total

                @pl.when(j > 0)
                def _():
                    send_out(j - 1)

                @pl.when(j > 1)
                def _():
                    combine(j - 2)
            else:
                oacc[...] += total
        row = (xs[j].astype(F32) + (oacc[...] + delta(lowm[0], bdbuf[:, pl.ds(o0, SUB)]))).astype(BF16)
        for q in range(blocks):
            back_send[:, j * blocks + q] = row[:, q * LANES:(q + 1) * LANES].reshape(groups, per_msg, PACK, LANES)
        for q in range(blocks):
            back_recv[j * blocks + q, mine_at] = back_send[me, j * blocks + q]

    run(at, n_out, n_kp, column)

    send_out(n_out - 1)
    combine(n_out - 2)
    combine(n_out - 1)

    for m, (c, count) in enumerate(messages):
        await_sent(send, c * blocks, count * blocks, xs_send.at[m])
    view = mask_send.at[pl.ds(0, per_msg * (groups - 1))]
    pltpu.make_async_copy(view, view, m_send).wait()
    for j in range(n_out):
        await_sent(back_send, j * blocks, blocks, b_send.at[j])
    pltpu.make_async_copy(out_own, out_own, o_sem).wait()


def solution(mesh):
    groups = mesh.shape["data"]
    row_spec = P(("rep", "data"), None)
    id_spec = P(("rep", "data"))
    owned_spec = P("data", None, None)

    def device_step(x, adapter_id, w_gate, w_up, w_down, a_gate, b_gate, a_up, b_up, a_down, b_down):
        tok, width = x.shape
        wide = w_gate.shape[1]
        per_owner, rank = a_gate.shape[:2]
        cap = (3 * tok + groups - 1) // groups
        rows, ranks = groups * cap, per_owner * rank
        per_msg, n_chunk, n_tile = cap // PACK, width // SUB, wide // SUB
        assert cap % PACK == 0 and width % (2 * SUB) == 0 and wide % (4 * SUB) == 0 and ranks == LANES

        def flat(m):
            return m.reshape(ranks, m.shape[2])

        vm = pltpu.VMEM
        any_spec = pl.BlockSpec(memory_space=pl.ANY)
        msg = (groups, width // LANES, per_msg, PACK, LANES)
        got = (width // LANES, groups * per_msg, PACK, LANES)
        small = (groups * per_msg, PACK, LANES)
        dma = pltpu.SemaphoreType.DMA
        return pl.pallas_call(
            functools.partial(layer_kernel, groups, cap, ALPHA / rank, per_owner, rank),
            out_shape=jax.ShapeDtypeStruct((tok, width), BF16),
            in_specs=[any_spec, pl.BlockSpec(memory_space=pltpu.VMEM)] + [any_spec] * 9,
            out_specs=any_spec,
            scratch_shapes=[
                vm((tok, width), BF16), vm(msg, BF16), vm(small, BF16), vm(got, BF16), vm(small, BF16),
                vm((n_chunk, rows, SUB), BF16), vm((2, 2 * HELD, rows, SUB), F32), vm((n_tile, rows, SUB), BF16),
                vm((PAIRS, 2, 2 * SUB, SUB), BF16), vm((n_chunk, 2 * ranks, SUB), BF16),
                vm((LBUFS, 3, ranks, SUB), BF16),
                vm((ranks, width), BF16), vm((rows, 2 * ranks), F32), vm((2, rows, ranks), BF16),
                vm((rows, ranks), F32), vm((rows, SUB), F32), vm(msg, BF16), vm(got, BF16),
                vm((width // SUB, tok, SUB), BF16), vm((tok, rows), BF16),
                dma((PAIRS,)), dma((2,)), dma((n_chunk,)), dma((LBUFS,)), dma((n_chunk,)), dma((n_chunk,)), dma, dma,
                dma((width // SUB,)), dma((width // SUB,)), dma,
            ],
            compiler_params=pltpu.CompilerParams(
                collective_id=0, has_side_effects=True, vmem_limit_bytes=67043328),
            name="owner_layer",
        )(x, adapter_id.reshape(1, tok), w_gate, w_up, w_down, flat(a_gate), flat(b_gate), flat(a_up), flat(b_up),
          flat(a_down), flat(b_down))

    return jax.shard_map(
        device_step, mesh=mesh,
        in_specs=(row_spec, id_spec, P(), P(), P()) + (owned_spec,) * 6,
        out_specs=row_spec, check_vma=False)
```

```python
import functools

import jax
import jax.numpy as jnp
from jax import lax
from jax.experimental import pallas as pl
from jax.experimental.pallas import tpu as pltpu
from jax.sharding import PartitionSpec as P

ALPHA = 32
MESH = pl.DeviceIdType.MESH
BF16, F32 = jnp.bfloat16, jnp.float32
SUB = 512
LANES = 128
PACK = 4
HELD = 9
PAIRS = 12
LBUFS = 4
LAG = 5
STEP = 3


def nt_dot(a, b):
    return lax.dot_general(a, b, (((1,), (1,)), ((), ())), preferred_element_type=F32)


def dot(a, b):
    return jnp.dot(a, b, preferred_element_type=F32)


def layer_kernel(
    groups, cap, scale, per_owner, rank,
    x_hbm, ids_ref, wg_hbm, wu_hbm, wd_hbm, ag_hbm, bg_hbm, au_hbm, bu_hbm, ad_hbm, bd_hbm,
    out_hbm,
    x_own, send, mask_send, recv, mask_recv, xs, acc, hid, wbuf, abuf, lbuf, bdbuf,
    low, lowm, lowd, oacc, back_send, back_recv, out_own, pick,
    w_sem, misc_sem, a_sem, l_sem, xs_send, xs_recv, m_send, m_recv, b_send, b_recv, o_sem,
):
    tok, width = x_own.shape
    rows = groups * cap
    wide = wg_hbm.shape[1]
    ranks = per_owner * rank
    n_chunk = width // SUB
    n_tile = wide // SUB
    n_out = width // SUB
    per_msg = cap // PACK
    blocks = SUB // LANES
    n_held = 2 * HELD
    k_pair = 4 * SUB
    n_kp = wide // k_pair
    n_deep = n_chunk // 2
    messages = [(0, 1), (1, 1)] + [(c, 2) for c in range(2, n_chunk, 2)]

    me = lax.axis_index("data")
    seen = []
    for d in range(groups // 4, 0, -1):
        for off in (2 * d, 2 * d + 1, groups - 2 * d, groups - 2 * d + 1):
            if off % groups and off % groups not in seen:
                seen.append(off % groups)
    seen += [off for off in range(1, groups) if off not in seen]
    peers = [lax.rem(me + off, groups) for off in seen]

    barrier = pltpu.get_barrier_semaphore()
    for peer in peers:
        pl.semaphore_signal(barrier, inc=1, device_id={"data": peer}, device_id_type=MESH)

    def nxt(slot):
        return jnp.where(slot == PAIRS - 1, 0, slot + 1)

    def start_a1(slot, c, n):
        for which, w in enumerate((wg_hbm, wu_hbm)):
            for half in range(2):
                n0 = pl.multiple_of(n * (2 * SUB) + half * SUB, SUB)
                pltpu.make_async_copy(
                    w.at[pl.ds(c * SUB, SUB), pl.ds(n0, SUB)],
                    wbuf.at[slot, which, pl.ds(half * SUB, SUB)], w_sem.at[slot],
                ).start()

    def start_gu(slot, p, n):
        k0 = pl.multiple_of(p * (2 * SUB), 2 * SUB)
        n0 = pl.multiple_of(n * SUB, SUB)
        for which, w in enumerate((wg_hbm, wu_hbm)):
            pltpu.make_async_copy(
                w.at[pl.ds(k0, 2 * SUB), pl.ds(n0, SUB)], wbuf.at[slot, which], w_sem.at[slot]).start()

    def start_d(slot, j, kp):
        n0 = pl.multiple_of(j * SUB, SUB)
        for half in range(2):
            k0 = pl.multiple_of(kp * k_pair + half * 2 * SUB, 2 * SUB)
            pltpu.make_async_copy(
                wd_hbm.at[pl.ds(k0, 2 * SUB), pl.ds(n0, SUB)], wbuf.at[slot, half], w_sem.at[slot]).start()

    def wait_w(slot):
        pltpu.make_async_copy(wbuf.at[slot], wbuf.at[slot], w_sem.at[slot]).wait()

    kinds = []
    for o in range(2):
        kinds += [("a1", o, n) for n in range(HELD)]
    for o in range(1, n_deep):
        kinds += [("gu", o, n) for n in range(n_held)]
    for n in range(n_held, n_tile):
        kinds += [("gb", n, o) for o in range(n_deep)]
    for o in range(n_out):
        kinds += [("d", o, n) for n in range(n_kp)]
    starts = {"a1": start_a1, "gu": start_gu, "gb": lambda slot, n, o: start_gu(slot, o, n), "d": start_d}
    inner = {"a1": HELD, "gu": n_held, "gb": n_deep, "d": n_kp}
    n_pair = len(kinds)

    def run(first, count, size, body):
        def ahead(step):
            items = [kinds[q] for q in range(first + step * size + PAIRS, first + (step + 1) * size + PAIRS)
                     if q < n_pair]
            return {k for k, _, _ in items}, items

        step = 0
        while step < count:
            names, items = ahead(step)
            end = step + 1
            if len(names) == 1:
                while end < count and (ahead(end)[0] == names or (names == {"d"} and not ahead(end)[0])):
                    end += 1
            guarded = names == {"d"}

            def one(s, carry, items=items, names=names, guarded=guarded, looped=end - step > 1):
                slot, o, n = carry
                slots = [slot]
                for _ in range(size - 1):
                    slots.append(nxt(slots[-1]))
                todo = []
                if looped:
                    kind = items[0][0]
                    for _ in range(size):
                        todo.append((kind, o, n))
                        wrap = n == inner[kind] - 1
                        o, n = jnp.where(wrap, o + 1, o), jnp.where(wrap, 0, n + 1)
                else:
                    todo = items

                def refill(i):
                    if i >= len(todo):
                        return
                    kind, oo, nn = todo[i]
                    if looped and guarded:
                        @pl.when(oo < n_out)
                        def _():
                            starts[kind](slots[i], oo, nn)
                    else:
                        starts[kind](slots[i], oo, nn)

                body(s, slots, refill)
                return nxt(slots[-1]), o, n

            slot0 = (first + step * size) % PAIRS
            _, o0, n0 = items[0] if items else (None, 0, 0)
            if end - step == 1:
                one(step, (jnp.int32(slot0), 0, 0))
            else:
                lax.fori_loop(step, end, one, (jnp.int32(slot0), jnp.int32(o0), jnp.int32(n0)))
            step = end

    def l_copies(n, s):
        n0 = pl.multiple_of(n * SUB, SUB)
        return [
            pltpu.make_async_copy(src.at[:, pl.ds(n0, SUB)], lbuf.at[s, i], l_sem.at[s])
            for i, src in enumerate((bg_hbm, bu_hbm, ad_hbm))
        ]

    x_copy = pltpu.make_async_copy(x_hbm, x_own, misc_sem.at[0])
    bd_copy = pltpu.make_async_copy(bd_hbm, bdbuf, misc_sem.at[1])
    x_copy.start()
    for i in range(2):
        for c in range(n_chunk):
            src = (ag_hbm, au_hbm)[i]
            pltpu.make_async_copy(
                src.at[:, pl.ds(c * SUB, SUB)], abuf.at[c, pl.ds(i * ranks, ranks)], a_sem.at[c]
            ).start()


    ids = ids_ref[...].astype(F32)
    r0 = lax.broadcasted_iota(jnp.int32, (tok, tok), 0).astype(F32)
    r1 = lax.broadcasted_iota(jnp.int32, (tok, tok), 1).astype(F32)
    ids_row = jnp.broadcast_to(ids, (tok, tok))
    ids_col = jnp.broadcast_to(jnp.sum(jnp.where(r0 == r1, ids_row, 0.0), axis=1, keepdims=True), (tok, tok))
    own_row = jnp.floor((ids_row + 0.5) * (1.0 / per_owner))
    own_col = jnp.floor((ids_col + 0.5) * (1.0 / per_owner))
    same = own_row == own_col
    arr_row = jnp.sum(jnp.where(same & (r0 < r1), 1.0, 0.0), axis=0, keepdims=True)
    arr_col = jnp.sum(jnp.where(same & (r1 < r0), 1.0, 0.0), axis=1, keepdims=True)
    slot_row = own_row[:1, :] * cap + arr_row
    slot_col = own_col[:, :1] * cap + arr_col
    loc_col = ids_col[:, :1] - own_col[:, :1] * per_owner
    s_row = lax.broadcasted_iota(jnp.int32, (rows, tok), 0).astype(F32)
    spread = jnp.where(s_row == jnp.broadcast_to(slot_row, (rows, tok)), 1.0, 0.0).astype(BF16)
    s_col = lax.broadcasted_iota(jnp.int32, (tok, rows), 1).astype(F32)
    pick[...] = jnp.where(s_col == jnp.broadcast_to(slot_col, (tok, rows)), 1.0, 0.0).astype(BF16)
    lane = lax.broadcasted_iota(jnp.int32, (tok, ranks), 1).astype(F32)
    lane_ad = jnp.floor((lane + 0.5) * (1.0 / rank))
    mine = jnp.where(lane_ad == jnp.broadcast_to(loc_col, (tok, ranks)), 1.0, 0.0).astype(BF16)

    mask_send[...] = dot(spread, mine).astype(BF16).reshape(mask_send.shape)
    x_copy.wait()
    for c in range(n_chunk):
        part = dot(spread, x_own[:, c * SUB:(c + 1) * SUB]).astype(BF16)
        for q in range(blocks):
            send[:, c * blocks + q] = part[:, q * LANES:(q + 1) * LANES].reshape(groups, per_msg, PACK, LANES)

    mine_at = pl.ds(per_msg * me, per_msg)

    def exchange(src, dst, first, count, send_sem, recv_sem):
        for peer in peers:
            pltpu.make_async_remote_copy(
                src_ref=src.at[peer, pl.ds(first, count)], dst_ref=dst.at[pl.ds(first, count), mine_at],
                send_sem=send_sem, recv_sem=recv_sem, device_id={"data": peer}, device_id_type=MESH,
            ).start()

    def send_out(j):
        exchange(back_send, back_recv, j * blocks, blocks, b_send.at[j], b_recv.at[j])

    def await_peers(buf, first, count, sem):
        view = buf.at[pl.ds(first, count), pl.ds(0, per_msg * (groups - 1))]
        pltpu.make_async_copy(view, view, sem).wait()

    def await_sent(buf, first, count, sem):
        view = buf.at[pl.ds(0, groups - 1), pl.ds(first, count)]
        pltpu.make_async_copy(view, view, sem).wait()

    @pl.loop(0, n_chunk * blocks)
    def _(q):
        recv[q, mine_at] = send[me, q]

    mask_recv[mine_at] = mask_send[mine_at]

    pl.semaphore_wait(barrier, groups - 1)

    for m, (c, count) in enumerate(messages):
        exchange(send, recv, c * blocks, count * blocks, xs_send.at[m], xs_recv.at[m])
    for peer in peers:
        pltpu.make_async_remote_copy(
            src_ref=mask_send.at[pl.ds(per_msg * peer, per_msg)], dst_ref=mask_recv.at[mine_at],
            send_sem=m_send, recv_sem=m_recv, device_id={"data": peer}, device_id_type=MESH,
        ).start()

    for i in range(PAIRS):
        starts[kinds[i][0]](i, kinds[i][1], kinds[i][2])
    for n in range(LBUFS):
        for cp in l_copies(n, n):
            cp.start()
    bd_copy.start()

    def arrive(m):
        first, count = messages[m]
        await_peers(recv, first * blocks, count * blocks, xs_recv.at[m])
        for c in range(first, first + count):
            for q in range(blocks):
                xs[c, :, q * LANES:(q + 1) * LANES] = recv[c * blocks + q].reshape(rows, LANES)
            pltpu.make_async_copy(abuf.at[c], abuf.at[c], a_sem.at[c]).wait()
            part = nt_dot(xs[c], abuf[c])
            low[...] = part if c == 0 else low[...] + part

    def masked(value):
        mask = mask_recv[...].reshape(rows, ranks).astype(F32) > 0.0
        return jnp.where(mask, value.astype(BF16).astype(F32), 0.0).astype(BF16)

    def delta(a, b):
        return (scale * dot(a, b)).astype(BF16).astype(F32)

    def deep(p):
        return jnp.concatenate([xs[2 * p], xs[2 * p + 1]], axis=1)

    def l_wait(s):
        pltpu.make_async_copy(lbuf.at[s], lbuf.at[s], l_sem.at[s]).wait()

    def finish(n, s, base):
        for p in range(2):
            cols = slice(p * SUB // 2, (p + 1) * SUB // 2)
            g = base(0, cols) + delta(lowm[0], lbuf[s, 0, :, cols])
            u = base(1, cols) + delta(lowm[1], lbuf[s, 1, :, cols])
            hid[n, :, cols] = (jax.nn.silu(g) * u).astype(BF16)
        lowd[...] += nt_dot(hid[n], lbuf[s, 2])

    def l_next(n, s):
        @pl.when(n + LBUFS < n_tile)
        def _():
            for cp in l_copies(n + LBUFS, s):
                cp.start()

    at = 0
    for c in range(2):
        arrive(c)

        def shallow(step, slots, refill, c=c):
            for slot in slots:
                wait_w(slot)
            for i, slot in enumerate(slots):
                for which in range(2):
                    for half in range(2):
                        part = dot(xs[c], wbuf[slot, which, half * SUB:(half + 1) * SUB])
                        n = 2 * (len(slots) * step + i) + half
                        if c == 0:
                            acc[which, n] = part
                        else:
                            acc[which, n] += part
                refill(i)

        run(at, HELD // STEP, STEP, shallow)
        at += HELD

    for p in range(1, n_deep):
        arrive(p + 1)
        last = p == n_deep - 1
        size = 2 if last else STEP
        if last:
            view = mask_recv.at[pl.ds(0, per_msg * (groups - 1))]
            pltpu.make_async_copy(view, view, m_recv).wait()
            for i in range(2):
                lowm[i] = masked(low[:, i * ranks:(i + 1) * ranks])
            lowd[...] = jnp.zeros_like(lowd)

        def some(step, slots, refill, p=p, last=last):
            for i, slot in enumerate(slots):
                wait_w(slot)
                if last:
                    l_wait(lax.rem(len(slots) * step + i, LBUFS))
            for i, slot in enumerate(slots):
                n = len(slots) * step + i
                if last:
                    s = lax.rem(n, LBUFS)
                    finish(n, s, lambda which, cols: acc[which, n, :, cols] + dot(deep(p), wbuf[slot, which, :, cols]))
                    l_next(n, s)
                else:
                    for which in range(2):
                        acc[which, n] += dot(deep(p), wbuf[slot, which])
                refill(i)

        run(at, n_held // size, size, some)
        at += n_held

    def whole(step, slots, refill):
        n = n_held + step
        s = lax.rem(n, LBUFS)
        for slot in slots:
            wait_w(slot)
        l_wait(s)

        def base(which, cols):
            total = dot(deep(0), wbuf[slots[0], which, :, cols])
            for p in range(1, n_deep):
                total = total + dot(deep(p), wbuf[slots[p], which, :, cols])
            return total

        finish(n, s, base)
        for i in range(len(slots)):
            refill(i)
        l_next(n, s)

    run(at, n_tile - n_held, n_deep, whole)
    at += (n_tile - n_held) * n_deep

    lowm[0] = masked(lowd[...])
    bd_copy.wait()

    def combine(j):
        await_peers(back_recv, j * blocks, blocks, b_recv.at[j])
        part = jnp.concatenate([back_recv[j * blocks + q].reshape(rows, LANES) for q in range(blocks)], axis=1)
        o0 = pl.multiple_of(j * SUB, SUB)
        out_own[j] = dot(pick[...], part).astype(BF16)
        pltpu.make_async_copy(out_own.at[j], out_hbm.at[:, pl.ds(o0, SUB)], o_sem).start()

    def column(j, slots, refill):
        @pl.when(j > 0)
        def _():
            send_out(j - 1)

        @pl.when(j >= LAG)
        def _():
            combine(j - LAG)

        cut = (n_kp + 1) // 2
        o0 = pl.multiple_of(j * SUB, SUB)
        for part, (lo, hi) in enumerate(((0, cut), (cut, n_kp))):
            total = None
            for kp in range(lo, hi):
                wait_w(slots[kp])
            for kp in range(lo, hi):
                for half in range(2):
                    h = 4 * kp + 2 * half
                    term = dot(jnp.concatenate([hid[h], hid[h + 1]], axis=1), wbuf[slots[kp], half])
                    total = term if total is None else total + term
            if part == 0:
                oacc[...] = total
            else:
                total = oacc[...] + total + delta(lowm[0], bdbuf[:, pl.ds(o0, SUB)])
                row = (xs[j].astype(F32) + total).astype(BF16)
                for q in range(blocks):
                    back_send[:, j * blocks + q] = row[:, q * LANES:(q + 1) * LANES].reshape(
                        groups, per_msg, PACK, LANES)
            for kp in range(lo, hi):
                refill(kp)
        for q in range(blocks):
            back_recv[j * blocks + q, mine_at] = back_send[me, j * blocks + q]

    run(at, n_out, n_kp, column)

    send_out(n_out - 1)

    @pl.loop(n_out - LAG, n_out)
    def _(j):
        combine(j)

    for m, (c, count) in enumerate(messages):
        await_sent(send, c * blocks, count * blocks, xs_send.at[m])
    view = mask_send.at[pl.ds(0, per_msg * (groups - 1))]
    pltpu.make_async_copy(view, view, m_send).wait()
    for j in range(n_out):
        await_sent(back_send, j * blocks, blocks, b_send.at[j])
    pltpu.make_async_copy(out_own, out_own, o_sem).wait()


def solution(mesh):
    groups = mesh.shape["data"]
    row_spec = P(("rep", "data"), None)
    id_spec = P(("rep", "data"))
    owned_spec = P("data", None, None)

    def device_step(x, adapter_id, w_gate, w_up, w_down, a_gate, b_gate, a_up, b_up, a_down, b_down):
        tok, width = x.shape
        wide = w_gate.shape[1]
        per_owner, rank = a_gate.shape[:2]
        cap = (3 * tok + groups - 1) // groups
        rows, ranks = groups * cap, per_owner * rank
        per_msg, n_chunk, n_tile = cap // PACK, width // SUB, wide // SUB
        assert cap % PACK == 0 and width % (2 * SUB) == 0 and wide % (4 * SUB) == 0 and ranks == LANES

        def flat(m):
            return m.reshape(ranks, m.shape[2])

        vm = pltpu.VMEM
        any_spec = pl.BlockSpec(memory_space=pl.ANY)
        msg = (groups, width // LANES, per_msg, PACK, LANES)
        got = (width // LANES, groups * per_msg, PACK, LANES)
        small = (groups * per_msg, PACK, LANES)
        dma = pltpu.SemaphoreType.DMA
        return pl.pallas_call(
            functools.partial(layer_kernel, groups, cap, ALPHA / rank, per_owner, rank),
            out_shape=jax.ShapeDtypeStruct((tok, width), BF16),
            in_specs=[any_spec, pl.BlockSpec(memory_space=pltpu.VMEM)] + [any_spec] * 9,
            out_specs=any_spec,
            scratch_shapes=[
                vm((tok, width), BF16), vm(msg, BF16), vm(small, BF16), vm(got, BF16), vm(small, BF16),
                vm((n_chunk, rows, SUB), BF16), vm((2, 2 * HELD, rows, SUB), F32), vm((n_tile, rows, SUB), BF16),
                vm((PAIRS, 2, 2 * SUB, SUB), BF16), vm((n_chunk, 2 * ranks, SUB), BF16),
                vm((LBUFS, 3, ranks, SUB), BF16),
                vm((ranks, width), BF16), vm((rows, 2 * ranks), F32), vm((2, rows, ranks), BF16),
                vm((rows, ranks), F32), vm((rows, SUB), F32), vm(msg, BF16), vm(got, BF16),
                vm((width // SUB, tok, SUB), BF16), vm((tok, rows), BF16),
                dma((PAIRS,)), dma((2,)), dma((n_chunk,)), dma((LBUFS,)), dma((n_chunk,)), dma((n_chunk,)), dma, dma,
                dma((width // SUB,)), dma((width // SUB,)), dma,
            ],
            compiler_params=pltpu.CompilerParams(
                collective_id=0, has_side_effects=True, vmem_limit_bytes=67043328),
            name="owner_layer",
        )(x, adapter_id.reshape(1, tok), w_gate, w_up, w_down, flat(a_gate), flat(b_gate), flat(a_up), flat(b_up),
          flat(a_down), flat(b_down))

    return jax.shard_map(
        device_step, mesh=mesh,
        in_specs=(row_spec, id_spec, P(), P(), P()) + (owned_spec,) * 6,
        out_specs=row_spec, check_vma=False)
```
